32 devices in a mesh: dom: 8 (over y, x, core), rep: 4 (over z).
Axes of the slice: x: 2, y: 2, z: 4, core: 2. Of those that a mesh axis runs over, the one named last changes fastest.
Arguments:
- right_sides: float32 [4, 48, 16, 384], P(None, 'dom', 'rep'), may hold values from -6 to 6
- diag_inverse: bfloat16 [4, 48, 384, 384], P(None, 'dom'), may hold values from -0.3125 to 0.3125
- panel_mats: bfloat16 [3, 512, 384, 384], P(None, ('dom', 'rep')), may hold values from -0.08984375 to 0.08984375
- panel_src: int32 [3, 512], P(None, ('dom', 'rep')), may hold values from 0 to 17, as said below
- panel_dst: int32 [3, 512], P(None, ('dom', 'rep')), may hold values from -1 to 47, as said below
Outputs:
- solution: float32 [4, 48, 16, 384], P(None, 'dom', 'rep')
The draws below stay inside these ranges and needn't reach their ends.
Inputs may be any that keep to these rules, and one draw needn't show every extreme that they name: `panel_src`: an entry of row l is below (l + 1) * 6, so the source tile lies in a level at most l; most of the entries lie in level l itself. A live entry of a list owned by dom index o names a tile of dom index (o + j) mod 8 with -2 <= j <= 2 or j = 4. Among the 16 entries of one device's list for one row, at most 3 live entries have the same destination dom index (panel_dst // 6), and in every list some dom index has exactly 3; lists of low dom indices tend to hold more live entries than those of high ones.
All inputs are finite; a program needn't handle non-finite values.
Results may differ from the reference program's by a relative error of at most 0.012.
Values may be sent and summed in bfloat16 or wider, within the bound.
A program may use at most 128 MiB of HBM per device.

```python
import jax
import jax.numpy as jnp
from jax import lax

CELLS = 128
NRHS = 16
TPL = 6
LEVELS = 4
HALF = 2
PPR = 16
TILES = 48
PANELS = 512
N_DOM = 8
N_REP = 4


def draw_panel_src(key, part):
    level_rows = LEVELS - 1
    entry_count = N_DOM * N_REP * PPR
    key_any, key_recent, key_choose = jax.random.split(jax.random.fold_in(key, 11), 3)
    row_index = jnp.arange(level_rows, dtype=jnp.int32)[:, None]
    anywhere = jax.random.randint(key_any, (level_rows, entry_count), 0, (row_index + 1) * TPL)
    recent = row_index * TPL + jax.random.randint(key_recent, (level_rows, entry_count), 0, TPL)
    chooser = jax.random.randint(key_choose, (level_rows, entry_count), 0, 2)
    return jnp.where(chooser == 0, recent, anywhere).astype(jnp.int32)


def draw_panel_dst(key, part):
    level_rows = LEVELS - 1
    block_count = N_DOM * N_REP
    hood = 2 * HALF + 2
    subkeys = jax.random.split(jax.random.fold_in(key, 23), 4)
    position = jnp.arange(PPR, dtype=jnp.int32)[None, None, :]
    owner = (jnp.arange(block_count, dtype=jnp.int32) // N_REP)[None, :, None]
    turn = jax.random.randint(subkeys[0], (level_rows, block_count, 1), 0, hood)
    klass = (position % hood + turn) % hood
    reach = jnp.where(klass == hood - 1, N_DOM // 2, klass - HALF)
    target = (owner + reach) % N_DOM
    dropper = jax.random.randint(subkeys[1], (level_rows, block_count, PPR), 0, 2 * N_DOM)
    padded = (position % hood != 0) & (dropper < owner + 1)
    column_slot = jax.random.randint(subkeys[2], (level_rows, block_count, PPR), 0, TPL)
    entries = jnp.where(padded, -1, target * TPL + column_slot)
    rotation = jax.random.randint(subkeys[3], (level_rows, block_count, 1), 0, PPR)
    reorder = (position + rotation) % PPR
    entries = jnp.take_along_axis(entries, reorder, axis=2)
    return entries.reshape(level_rows, block_count * PPR).astype(jnp.int32)


def block_levels(stream_key, extent, cuts, least, largest):
    gain, own = 1.0, jax.random.fold_in(stream_key, 6)
    for dim, blocks in cuts:
        heights = jnp.exp(jax.random.uniform(jax.random.fold_in(own, dim), (blocks,), jnp.float32, least / len(cuts), largest / len(cuts)))
        gain = gain * jnp.repeat(heights, extent[dim] // blocks).reshape([-1 if axis == dim else 1 for axis in range(len(extent))])
    return gain


def gaussian(key, extent, spread, limit, cuts=(), held_as=jnp.bfloat16):
    values = jax.random.normal(key, extent, jnp.float32) * spread
    if len(cuts) > 0:
        values = block_levels(key, extent, cuts, -0.22, 0.18) * values
    return jnp.clip(values, min=-limit, max=limit).astype(held_as)


def setup_inputs(seed: int = 0) -> dict:
    key_list = jax.random.split(jax.random.key(seed), 6)
    right_sides = gaussian(key_list[0], (LEVELS, TILES, NRHS, 3 * CELLS), 1.0, 6.0, ((1, 8), (2, 4)), jnp.float32)
    diag_inverse = gaussian(key_list[1], (LEVELS, TILES, 3 * CELLS, 3 * CELLS), (3 * CELLS) ** -0.5, 0.3125, ((1, 8),))
    panel_mats = gaussian(key_list[2], (LEVELS - 1, PANELS, 3 * CELLS, 3 * CELLS), 0.015, 0.08984375, ((1, 32),))
    panel_src = draw_panel_src(jax.random.fold_in(key_list[5], 71), 0)
    panel_dst = draw_panel_dst(jax.random.fold_in(key_list[5], 71), 0)
    return {"right_sides": right_sides, "diag_inverse": diag_inverse, "panel_mats": panel_mats, "panel_src": panel_src, "panel_dst": panel_dst}


def reference(right_sides, diag_inverse, panel_mats, panel_src, panel_dst):
    highest = lax.Precision.HIGHEST
    tile_total = N_DOM * TPL
    owner_dom = jnp.arange(N_DOM * N_REP * PPR, dtype=jnp.int32) // (N_REP * PPR)
    solved_all = []
    for level_index in range(LEVELS):
        residual = right_sides[level_index]
        if level_index > 0:
            history = jnp.stack([entry.astype(jnp.bfloat16) for entry in solved_all])
            source_ids = panel_src[level_index - 1]
            source_level = (source_ids // TPL).astype(jnp.int32)
            source_pos = (owner_dom * TPL + source_ids % TPL).astype(jnp.int32)
            sources = history[source_level, source_pos]
            contribution = jnp.einsum('qcx,qxy->qcy', sources.astype(jnp.float32), panel_mats[level_index - 1].astype(jnp.float32), precision=highest)
            onehot = (panel_dst[level_index - 1][:, None] == jnp.arange(tile_total, dtype=jnp.int32)[None, :]).astype(jnp.float32)
            incoming = jnp.einsum('qt,qcy->tcy', onehot, contribution, precision=highest)
            residual = residual - incoming
        rounded = lax.optimization_barrier(residual.astype(jnp.bfloat16))
        solved = jnp.einsum('tcx,txy->tcy', rounded.astype(jnp.float32), diag_inverse[level_index].astype(jnp.float32), precision=highest)
        solved_all.append(solved)
    return jnp.stack(solved_all)
```

```python
import functools

import jax
import jax.numpy as jnp
import numpy as np
from jax import lax
from jax.experimental import pallas as pl
from jax.experimental.pallas import tpu as pltpu
from jax.sharding import PartitionSpec as P

HALF = 2
SLOTS = 3
HOOD = 2 * HALF + 2
MESH = pl.DeviceIdType.MESH
F32 = jnp.float32
BF16 = jnp.bfloat16


def round_up(value, unit):
    return -(-value // unit) * unit


def iota(shape, dim):
    return lax.broadcasted_iota(jnp.int32, shape, dim).astype(F32)


def lane_tables(rep_size, panel_count, col_count, slot_rows):
    rhs = rep_size * col_count
    width = max(panel_count * rhs, HOOD * rep_size * slot_rows, 128)
    lane = np.arange(width)
    return np.stack(
        [
            lane // rhs,
            (lane % rhs) // col_count * slot_rows + lane % col_count,
            lane // slot_rows,
            (lane % slot_rows) // col_count,
            lane % col_count,
            lane % slot_rows,
            0 * lane,
            0 * lane,
        ]
    ).astype(np.float32)


def regroup_table(rep_size, tile_count, col_count, group_rows):
    table = np.zeros((tile_count * rep_size * col_count, rep_size * group_rows), np.float32)
    for r in range(rep_size):
        for t in range(tile_count):
            for c in range(col_count):
                table[(t * rep_size + r) * col_count + c, r * group_rows + t * col_count + c] = 1
    return table


def kernel(
    dims,
    src_ref, dst_ref, rs_ref, lanes_ref, regroup_ref, diag_hbm, panel_hbm,
    out_ref,
    diag, panel, store, contrib, pack, unpack,
    solved_send, solved_recv, val_send, val_recv, id_send, id_recv,
    diag_sem, panel_sem, solved_ssem, solved_rsem, val_ssem, val_rsem, id_ssem, id_rsem,
):
    levels, tiles, cols, width, panels, dom_size, rep_size, slot_rows, group_rows, chunk = dims
    far = dom_size // 2
    rhs = rep_size * cols
    tile_rows = tiles * cols
    me_d = lax.axis_index("dom")
    me_r = lax.axis_index("rep")
    offsets = [o - HALF for o in range(HOOD - 1)] + [far]
    senders = HOOD * rep_size

    def peer_dom(offset):
        return lax.rem(me_d + (offset + dom_size), dom_size)

    def peer_rep(step):
        return lax.rem(me_r + step, rep_size)

    peers = [
        (j, step)
        for j in (HOOD - 1, 0, HOOD - 2, 1, HOOD - 3, HALF)
        for step in range(rep_size - 1, -1, -1)
        if (offsets[j], step) != (0, 0)
    ]

    def load_diag(level):
        return pltpu.make_async_copy(diag_hbm.at[level], diag.at[level], diag_sem.at[level])

    def load_panel(level, part):
        span = pl.ds(part * chunk, chunk)
        return pltpu.make_async_copy(
            panel_hbm.at[level, span], panel.at[level, span], panel_sem.at[level, part]
        )

    def send_id(j, step):
        return pltpu.make_async_remote_copy(
            src_ref=id_send.at[j],
            dst_ref=id_recv.at[j * rep_size + me_r],
            send_sem=id_ssem.at[j * rep_size + step],
            recv_sem=id_rsem.at[j * rep_size + me_r],
            device_id=(peer_dom(offsets[j]), peer_rep(step)),
            device_id_type=MESH,
        )

    def await_id(j, step):
        slot = j * rep_size + peer_rep(step)
        pltpu.make_async_remote_copy(
            src_ref=id_send.at[j],
            dst_ref=id_recv.at[slot],
            send_sem=id_ssem.at[j * rep_size + step],
            recv_sem=id_rsem.at[slot],
            device_id=(peer_dom(-offsets[j]), peer_rep(step)),
            device_id_type=MESH,
        ).wait_recv()


    def send_val(level, j, step):
        return pltpu.make_async_remote_copy(
            src_ref=val_send.at[level, j * rep_size + peer_rep(step)],
            dst_ref=val_recv.at[level, j * rep_size + me_r],
            send_sem=val_ssem.at[level, j * rep_size + step],
            recv_sem=val_rsem.at[level, j * rep_size + me_r],
            device_id=(peer_dom(offsets[j]), peer_rep(step)),
            device_id_type=MESH,
        )

    def await_val(level, j, step):
        slot = j * rep_size + peer_rep(step)
        pltpu.make_async_remote_copy(
            src_ref=val_send.at[level, slot],
            dst_ref=val_recv.at[level, slot],
            send_sem=val_ssem.at[level, j * rep_size + step],
            recv_sem=val_rsem.at[level, slot],
            device_id=(peer_dom(-offsets[j]), peer_rep(step)),
            device_id_type=MESH,
        ).wait_recv()

    tile_span = pl.ds(0, tile_rows)

    def send_solved(level, step):
        return pltpu.make_async_remote_copy(
            src_ref=solved_send.at[level, tile_span],
            dst_ref=solved_recv.at[level, me_r, tile_span],
            send_sem=solved_ssem.at[level, step],
            recv_sem=solved_rsem.at[level, me_r],
            device_id=(me_d, peer_rep(step)),
            device_id_type=MESH,
        )

    def await_solved(level, step):
        slot = peer_rep(step)
        pltpu.make_async_remote_copy(
            src_ref=solved_send.at[level, tile_span],
            dst_ref=solved_recv.at[level, slot, tile_span],
            send_sem=solved_ssem.at[level, step],
            recv_sem=solved_rsem.at[level, slot],
            device_id=(me_d, slot),
            device_id_type=MESH,
        ).wait_recv()

    load_diag(0).start()

    solved_recv[...] = jnp.zeros_like(solved_recv)

    barrier = pltpu.get_barrier_semaphore()
    for j, step in peers:
        pl.semaphore_signal(
            barrier,
            inc=1,
            device_id=(peer_dom(offsets[j]), peer_rep(step)),
            device_id_type=MESH,
        )

    def route():
        owner = me_d.astype(F32)
        lane_panel = lanes_ref[0:1, : panels * rhs]
        lane_row = lanes_ref[1:2, : panels * rhs]
        id_level = lanes_ref[2:3, :128]
        id_slot = lanes_ref[3:4, :128]
        id_col = lanes_ref[4:5, :128]
        row16 = iota((panels, panels), 0)
        col16 = iota((panels, panels), 1)
        wanted = [jnp.zeros((1, 128), F32) for _ in range(HOOD)]
        for l in range(levels - 1):
            drow = dst_ref[l : l + 1, :].astype(F32)
            dcol = jnp.sum(jnp.where(row16 == col16, drow, 0.0), axis=1, keepdims=True)
            trow = jnp.where(drow >= 0, jnp.floor((drow + 0.5) * (1.0 / tiles)), -1.0)
            tcol = jnp.where(dcol >= 0, jnp.floor((dcol + 0.5) * (1.0 / tiles)), -1.0)
            earlier = (tcol == trow) & (drow >= 0) & (col16 < row16)
            rank = jnp.sum(jnp.where(earlier, 1.0, 0.0), axis=1, keepdims=True)
            away = tcol - owner
            away = away + jnp.where(away < 0, float(dom_size), 0.0)
            near = away + HALF
            near = near - jnp.where(near >= dom_size, float(dom_size), 0.0)
            reach = jnp.where(away == far, float(HOOD - 1), near)
            reach = jnp.where(dcol >= 0, reach, -1.0)
            place = jnp.where(
                dcol >= 0, reach * (rep_size * slot_rows) + rank * cols, -1.0e6
            )
            tile = dcol - tiles * tcol
            spread = jnp.where(iota((panels, panels * rhs), 0) == lane_panel, place, 0.0)
            goal = jnp.sum(spread, axis=0, keepdims=True) + lane_row
            pack[l] = jnp.where(
                iota((senders * slot_rows, panels * rhs), 0) == goal, 1.0, 0.0
            ).astype(BF16)
            mine = (rank == id_slot) & (id_level == l)
            for j in range(HOOD):
                found = jnp.where(mine & (reach == j), tile + 1.0, 0.0)
                wanted[j] = wanted[j] + jnp.sum(found, axis=0, keepdims=True)
        for j in range(HOOD):
            row = jnp.where(wanted[j] > 0, (wanted[j] - 1.0) * cols + id_col, -1.0)
            id_send[j] = row.astype(jnp.int32)
        id_recv[HALF * rep_size + me_r] = id_send[HALF]

    def learn_ids():
        for j, step in peers:
            await_id(j, step)
        row_of = iota((senders, 128), 0)
        ids = jnp.zeros((senders, 128), F32)
        for s in range(senders):
            ids = jnp.where(row_of == s, id_recv[s].astype(F32), ids)
        ids = ids.astype(BF16)
        span = senders * slot_rows
        lane_sender = lanes_ref[2:3, :span]
        lane_in = lanes_ref[5:6, :span]
        for l in range(levels - 1):
            take = jnp.where(iota((128, span), 0) == lane_in + l * slot_rows, 1.0, 0.0)
            every = jnp.dot(ids, take.astype(BF16), preferred_element_type=F32)
            own = jnp.where(iota((senders, span), 0) == lane_sender, every, 0.0)
            goal = jnp.sum(own, axis=0, keepdims=True)
            unpack[l] = jnp.where(iota((tile_rows, span), 0) == goal, 1.0, 0.0).astype(BF16)

    def solve(level, residual):
        row_tile = lax.broadcasted_iota(jnp.int32, (tile_rows, width), 0)
        total = jnp.zeros((tile_rows, width), F32)
        for t in range(tiles):
            inside = (row_tile >= t * cols) & (row_tile < (t + 1) * cols)
            part = jnp.where(inside, residual, 0.0).astype(BF16)
            total = total + jnp.dot(part, diag[level, t], preferred_element_type=F32)
        return total

    route()
    pl.semaphore_wait(barrier, len(peers))

    for level in range(levels):
        residual = rs_ref[level]
        if level > 0:
            for j, step in peers:
                await_val(level - 1, j, step)
            arrived = val_recv[level - 1].reshape(senders * slot_rows, width)
            residual = residual - jnp.dot(
                unpack[level - 1], arrived, preferred_element_type=F32
            )
        load_diag(level).wait()
        solved = solve(level, residual)
        out_ref[level] = solved
        if level + 1 == levels:
            break
        rounded = solved.astype(BF16)
        solved_send[level, tile_span] = rounded
        for step in range(1, rep_size):
            send_solved(level, step).start()
        solved_recv[level, me_r, tile_span] = rounded
        if level == 0:
            for part in range(panels // chunk):
                load_panel(0, part).start()
            for j, step in peers:
                send_id(j, step).start()
        for step in range(1, rep_size):
            await_solved(level, step)
        gathered = jnp.dot(
            regroup_ref[...],
            solved_recv[level].reshape(rep_size * group_rows, width),
            preferred_element_type=F32,
        ).astype(BF16)
        store[level * tiles : (level + 1) * tiles] = gathered.reshape(tiles, rhs, width)
        for part in range(panels // chunk):
            load_panel(level, part).wait()
            for p in range(part * chunk, (part + 1) * chunk):
                source = store[src_ref[level, p]]
                product = jnp.dot(source, panel[level, p], preferred_element_type=F32)
                contrib[p * rhs : (p + 1) * rhs] = product.astype(BF16)
        packed = jnp.dot(pack[level], contrib[...], preferred_element_type=F32).astype(BF16)
        val_send[level] = packed.reshape(senders, slot_rows, width)
        for j, step in peers:
            send_val(level, j, step).start()
        own_slot = HALF * rep_size + me_r
        val_recv[level, own_slot] = val_send[level, own_slot]
        load_diag(level + 1).start()
        if level + 2 < levels:
            for part in range(panels // chunk):
                load_panel(level + 1, part).start()
        if level == 0:
            learn_ids()

    for j, step in peers:
        send_id(j, step).wait_send()
        for level in range(levels - 1):
            send_val(level, j, step).wait_send()
    for step in range(1, rep_size):
        for level in range(levels - 1):
            send_solved(level, step).wait_send()


def per_device(right_sides, diag_inverse, panel_mats, panel_src, panel_dst):
    levels, tiles, cols, width = right_sides.shape
    panels = panel_mats.shape[1]
    dom_size = lax.axis_size("dom")
    rep_size = lax.axis_size("rep")
    rhs = rep_size * cols
    tile_rows = tiles * cols
    slot_rows = round_up(SLOTS * cols, 16)
    group_rows = round_up(tile_rows, 16)
    senders = HOOD * rep_size
    chunk = 4 if panels % 4 == 0 else 1
    assert (levels - 1) * slot_rows <= 128
    dims = (
        levels, tiles, cols, width, panels, dom_size, rep_size, slot_rows, group_rows, chunk
    )
    lanes = jnp.asarray(lane_tables(rep_size, panels, cols, slot_rows))
    regroup = jnp.asarray(regroup_table(rep_size, tiles, cols, group_rows), BF16)
    vmem = pl.BlockSpec(memory_space=pltpu.VMEM)
    hbm = pl.BlockSpec(memory_space=pl.ANY)
    dma = pltpu.SemaphoreType.DMA
    solved = pl.pallas_call(
        functools.partial(kernel, dims),
        out_shape=jax.ShapeDtypeStruct((levels, tile_rows, width), F32),
        in_specs=[pl.BlockSpec(memory_space=pltpu.SMEM), vmem, vmem, vmem, vmem, hbm, hbm],
        out_specs=vmem,
        scratch_shapes=[
            pltpu.VMEM(diag_inverse.shape, BF16),
            pltpu.VMEM(panel_mats.shape, BF16),
            pltpu.VMEM(((levels - 1) * tiles, rhs, width), BF16),
            pltpu.VMEM((panels * rhs, width), BF16),
            pltpu.VMEM((levels - 1, senders * slot_rows, panels * rhs), BF16),
            pltpu.VMEM((levels - 1, tile_rows, senders * slot_rows), BF16),
            pltpu.VMEM((levels - 1, group_rows, width), BF16),
            pltpu.VMEM((levels - 1, rep_size, group_rows, width), BF16),
            pltpu.VMEM((levels - 1, senders, slot_rows, width), BF16),
            pltpu.VMEM((levels - 1, senders, slot_rows, width), BF16),
            pltpu.VMEM((HOOD, 1, 128), jnp.int32),
            pltpu.VMEM((senders, 1, 128), jnp.int32),
            dma((levels,)),
            dma((levels - 1, panels // chunk)),
            dma((levels - 1, rep_size)),
            dma((levels - 1, rep_size)),
            dma((levels - 1, senders)),
            dma((levels - 1, senders)),
            dma((senders,)),
            dma((senders,)),
        ],
        compiler_params=pltpu.CompilerParams(
            collective_id=0, has_side_effects=True, vmem_limit_bytes=56 * 1024 * 1024
        ),
    )(
        panel_src,
        panel_dst,
        right_sides.reshape(levels, tile_rows, width),
        lanes,
        regroup,
        diag_inverse,
        panel_mats,
    )
    return solved.reshape(right_sides.shape)


def solution(mesh):
    return jax.shard_map(
        per_device,
        mesh=mesh,
        in_specs=(
            P(None, "dom", "rep", None),
            P(None, "dom", None, None),
            P(None, ("dom", "rep"), None, None),
            P(None, ("dom", "rep")),
            P(None, ("dom", "rep")),
        ),
        out_specs=P(None, "dom", "rep", None),
        check_vma=False,
    )
```
